256 devices in a mesh: row: 16 (over z, x_lo), col: 8 (over y, x_hi), depth: 2 (over core).
Axes of the slice: x: 4 (x_hi: 2, x_lo: 2; x = x_hi * 2 + x_lo), y: 4, z: 8, core: 2. Of those that a mesh axis runs over, the one named last changes fastest.
Arguments:
- tokens: bfloat16 [2048, 5376], P('row', 'depth'), may hold values from -6 to 6
- gate_weight: bfloat16 [9216, 5376], P(('col', 'row'), 'depth'), may hold values from -0.078125 to 0.078125
- up_weight: bfloat16 [9216, 5376], P(('col', 'row'), 'depth'), may hold values from -0.078125 to 0.078125
- down_weight: bfloat16 [9216, 5376], P(('col', 'depth'), 'row'), may hold values from -0.09375 to 0.09375
Outputs:
- output: bfloat16 [2048, 5376], P('row', ('col', 'depth'))
The draws below stay inside these ranges and needn't reach their ends.
All inputs are finite; a program needn't handle non-finite values.
Results may differ from the reference program's by a relative error of at most 0.0049.
Values may be sent and summed in bfloat16 or wider, within the bound.
No kernel may reach another device: no remote copies, remote signals or barrier semaphores. Data moves between devices by JAX's collectives and lax.ppermute only.
A program may use at most 64 MiB of HBM per device.

```python
import jax
import jax.numpy as jnp

D = 5376
FFW = 9216
TOKENS = 2048


def strengthened(result, key, source, target, parts, factor):
    def block_of(dim):
        return (jnp.arange(result.shape[dim]) // (result.shape[dim] // parts)).reshape((-1,) + (1,) * (result.ndim - 1 - dim))

    one_side = jax.random.permutation(key, parts)[block_of(target)]
    second = (block_of(target) + parts // 2) % parts
    return jnp.where((block_of(source) == one_side) | (block_of(source) == second), factor * result, result)


def level_of(own_key, extent, split, smallest, largest):
    factor_of, own = 1.0, jax.random.fold_in(own_key, 6)
    for axis_at, blocks in split:
        draws = jnp.exp(jax.random.uniform(jax.random.fold_in(own, axis_at), (blocks,), jnp.float32, smallest / len(split), largest / len(split)))
        factor_of = factor_of * jnp.repeat(draws, extent[axis_at] // blocks).reshape([-1 if axis == axis_at else 1 for axis in range(len(extent))])
    return factor_of


def gaussian(rng, dims, spread, limit, pieces=(), held_as=jnp.bfloat16):
    loudness = level_of(rng, dims, pieces, -0.22, 0.18) if pieces else 1.0
    result = jax.random.normal(rng, dims, jnp.float32) * spread * loudness
    return jnp.minimum(jnp.maximum(result, -limit), limit).astype(held_as)


def noise_with(key, dims, spread, most, shards, heavy, dtype=jnp.bfloat16):
    result = spread * jax.random.normal(key, dims, jnp.float32)
    if shards:
        result = result * level_of(key, dims, shards, -0.22, 0.18)
    return jnp.clip(strengthened(result, jax.random.fold_in(key, 3), *heavy), -most, most).astype(dtype)


def setup_inputs(seed: int = 0) -> dict:
    key_of = jax.random.split(jax.random.key(seed), 5)
    tokens = gaussian(key_of[0], (TOKENS, D), 1.0, 6.0, ((0, 16), (1, 2)))
    gate_weight = gaussian(key_of[1], (FFW, D), D ** -0.5, 0.078125, ((0, 128), (1, 2)))
    up_weight = gaussian(key_of[2], (FFW, D), D ** -0.5, 0.078125, ((0, 128), (1, 2)))
    down_weight = noise_with(key_of[3], (FFW, D), FFW ** -0.5, 0.09375, ((0, 16), (1, 16)), (0, 1, 16, 2.0))
    return dict(tokens=tokens, gate_weight=gate_weight, up_weight=up_weight, down_weight=down_weight)


def reference(tokens, gate_weight, up_weight, down_weight):
    gate_part = jnp.dot(tokens, gate_weight.T, preferred_element_type=jnp.float32)
    up_part = jnp.dot(tokens, up_weight.T, preferred_element_type=jnp.float32)
    hidden = (jax.nn.silu(gate_part) * up_part).astype(jnp.bfloat16)
    return jnp.dot(hidden, down_weight, preferred_element_type=jnp.float32).astype(jnp.bfloat16)
```

```python
import jax
import jax.numpy as jnp
from jax import lax
from jax.experimental import pallas as pl
from jax.experimental.pallas import tpu as pltpu
from jax.sharding import Mesh, PartitionSpec as P


Z, XL, Y, XH, C = 8, 2, 4, 2, 2
X_FWD = [((x % 2) * 2 + x // 2, (((x + 1) % 4) % 2) * 2 + ((x + 1) % 4) // 2) for x in range(4)]
X_BWD = [(b, a) for a, b in X_FWD]
PAD = 384


def ring(n, k):
    return [(i, (i + k) % n) for i in range(n)]


def py(v, k):
    return lax.ppermute(v, "y", ring(Y, k))


def pz(v, k):
    return lax.ppermute(v, "z", ring(Z, k))


def swap(v, axis):
    return lax.ppermute(v, axis, [(0, 1), (1, 0)])


def z_ring(block):
    half = block.shape[0] // 2
    ups, downs = [block], [block]
    for _ in range(3):
        ups.append(pz(ups[-1], 1))
        downs.append(pz(downs[-1], -1))
    return ups + downs[1:] + [pz(ups[-1][:half], 1), pz(downs[-1][half:], -1)]


def first_kernel(pos, *refs):
    blocks, (u4, d4), weights = refs[:7], refs[7:9], refs[9:14]
    keep, send, tok, wts = refs[14:]
    z, xl, c = pos[0], pos[1], pos[2]
    n = blocks[0].shape[0] // 2

    def base(src):
        src = lax.rem(src + Z, Z)
        return (((src // 4) ^ c) * 4 + lax.rem(src, 4)) * (2 * n)

    def put(at, part, rows):
        tok[pl.ds(pl.multiple_of(at + part * n, n), n), :] = rows

    for block, off in zip(blocks, (0, -1, -2, -3, 1, 2, 3)):
        at = base(z + off)
        put(at, xl, block[:n, :])
        put(at, 1 - xl, block[n:, :])
    at = base(z + 4)
    put(at, xl, u4[...])
    put(at, 1 - xl, d4[...])
    row = 0
    for w in weights:
        wts[row:row + w.shape[0], :] = w[...]
        row += w.shape[0]
    for out, lo in ((send, 256), (keep, 0)):
        out[...] = lax.dot_general(wts[...], tok[lo:lo + 256, :], (((1,), (1,)), ((), ())),
                                   preferred_element_type=jnp.float32)


def second_kernel(pos, *refs):
    blocks, (u4, d4), (near, far) = refs[:7], refs[7:9], refs[9:11]
    out, hid = refs[11:]
    z, c = pos[0], pos[2]
    rows = blocks[0].shape[0]

    def base(src):
        src = lax.rem(src + Z, Z)
        return (((src // 4) ^ c) * 4 + lax.rem(src, 4)) * rows

    for block, off in zip(blocks, (0, -1, -2, -3, 1, 2, 3)):
        hid[pl.ds(pl.multiple_of(base(z + off), 32), rows), :] = block[...]
    at = base(z + 4)
    hid[pl.ds(pl.multiple_of(at, 16), rows // 2), :] = u4[...]
    hid[pl.ds(pl.multiple_of(at + rows // 2, 16), rows // 2), :] = d4[...]
    dims = (((0,), (0,)), ((), ()))
    k = 4 * rows
    for d in range(2):
        cols = slice(d * PAD, (d + 1) * PAD)
        val = lax.dot_general(hid[:k, :], near[:, cols], dims, preferred_element_type=jnp.float32)
        val += lax.dot_general(hid[k:, :], far[:, cols], dims, preferred_element_type=jnp.float32)
        val = val.astype(out.dtype)
        for zj in range(4):
            for xl in range(2):
                out[xl * 8 + zj * 2 + d] = val[(zj * 2 + xl) * 32:(zj * 2 + xl) * 32 + 32, :]


def vmem(n):
    return [pl.BlockSpec(memory_space=pltpu.VMEM)] * n


def solution(mesh):
    grid = Mesh(mesh.devices.reshape(Z, XL, Y, XH, C), ("z", "xl", "y", "xh", "c"))
    final_axes = ("z", "y", "xh", "c")
    final_perm = []
    for z in range(Z):
        for y in range(Y):
            for xh in range(XH):
                for c in range(C):
                    src = ((z * Y + y) * XH + xh) * C + c
                    dst = (((4 * c + y) * Y + z // 2) * XH + z % 2) * C + xh
                    final_perm.append((src, dst))

    def body(tokens, gate, up, down):
        z, xl, y, c = (lax.axis_index(a) for a in ("z", "xl", "y", "c"))
        pos = jnp.stack([z, xl, c]).astype(jnp.int32)

        w = jnp.concatenate([gate, up], 0)
        units = gate.shape[0]
        w_m1, w_p1 = py(w, 1), py(w, -1)
        w_g2, w_u2 = py(w_m1[:units], 1), py(w_p1[units:], -1)

        n = tokens.shape[0] // Y
        mine = lax.dynamic_slice_in_dim(tokens, y * n, n, 0)
        opp_a = lax.ppermute(mine[:n // 2], ("xl", "xh"), X_FWD)
        opp_b = lax.ppermute(mine[n // 2:], ("xl", "xh"), X_BWD)
        toks = z_ring(jnp.concatenate([mine, opp_a, opp_b], 0))

        dw = jnp.pad(down, ((0, 0), (0, PAD - down.shape[1]))).reshape(4, XL, units, PAD)
        own = lax.dynamic_index_in_dim(dw, xl, 1, False).reshape(4 * units, PAD)
        other = lax.dynamic_index_in_dim(dw, 1 - xl, 1, False).reshape(4 * units, PAD)
        got = swap(other, "xl")
        dblk = jnp.where(xl == 0, jnp.concatenate([own, got], 1), jnp.concatenate([got, own], 1))
        parts = [dblk, py(dblk, 1), py(dblk, -1), py(dblk, 2)]
        near = jnp.stack([p.reshape(4, units, 2 * PAD) for p in parts], 1).reshape(-1, 2 * PAD)
        far = swap(near, "c")

        m, t, k = 8 * units, 2 * Z * n, tokens.shape[1]
        half = jax.ShapeDtypeStruct((m, t // 2), jnp.float32)
        keep, send = pl.pallas_call(
            first_kernel,
            out_shape=(half, half),
            in_specs=[pl.BlockSpec(memory_space=pltpu.SMEM)] + vmem(14),
            out_specs=tuple(vmem(2)),
            scratch_shapes=[pltpu.VMEM((t, k), jnp.bfloat16), pltpu.VMEM((m, k), jnp.bfloat16)],
            compiler_params=pltpu.CompilerParams(vmem_limit_bytes=40 << 20),
            cost_estimate=pl.CostEstimate(flops=2 * m * t * k, bytes_accessed=2 * k * (m + t), transcendentals=0),
            name="first",
        )(pos, *toks, w, w_m1, w_p1, w_g2, w_u2)
        whole = (keep + swap(send, "c")).reshape(Y, 2, units, t // 2)
        g, u = whole[:, 0], whole[:, 1]
        hidden = (jax.nn.silu(g) * u).astype(jnp.bfloat16).reshape(Y * units, t // 2)

        hids = z_ring(hidden)
        shares = pl.pallas_call(
            second_kernel,
            out_shape=jax.ShapeDtypeStruct((16, n, PAD), jnp.bfloat16),
            in_specs=[pl.BlockSpec(memory_space=pltpu.SMEM)] + vmem(11),
            out_specs=vmem(1)[0],
            scratch_shapes=[pltpu.VMEM((Z * Y * units, t // 2), jnp.bfloat16)],
            compiler_params=pltpu.CompilerParams(vmem_limit_bytes=24 << 20),
            cost_estimate=pl.CostEstimate(flops=2 * Z * Y * units * t * PAD, bytes_accessed=6 << 20, transcendentals=0),
            name="second",
        )(pos, *hids, near, far)

        swapped = lax.all_to_all(shares, ("xl", "y", "xh"), 0, 0, tiled=True)
        swapped = swapped.reshape(XL, Y, XH, n, PAD).astype(jnp.float32)
        total = swapped.sum((0, 2)).astype(jnp.bfloat16).reshape(Y * n, PAD)
        total = lax.ppermute(total, final_axes, final_perm)
        return total[:, :down.shape[1]]

    row, col = ("z", "xl"), ("y", "xh")
    f = jax.shard_map(
        body,
        mesh=grid,
        in_specs=(P(row, "c"), P(col + row, "c"), P(col + row, "c"), P(col + ("c",), row)),
        out_specs=P(row, col + ("c",)),
        check_vma=False,
    )
    return f
```

```python
import jax
import jax.numpy as jnp
from jax import lax
from jax.experimental import pallas as pl
from jax.experimental.pallas import tpu as pltpu
from jax.sharding import Mesh, PartitionSpec as P


Z, XL, Y, XH, C = 8, 2, 4, 2, 2
PAD = 384
OFFSETS = (0, -1, -2, -3, 1, 2, 3)


def ring(n, k):
    return [(i, (i + k) % n) for i in range(n)]


def x_ring(k):
    at = [(x % 2) * 2 + x // 2 for x in range(4)]
    return [(at[a], at[b]) for a, b in ring(4, k)]


def px(v, k):
    return lax.ppermute(v, ("xl", "xh"), x_ring(k))


def py(v, k):
    return lax.ppermute(v, "y", ring(Y, k))


def pz(v, k):
    return lax.ppermute(v, "z", ring(Z, k))


def core_swap(v):
    return lax.ppermute(v, "c", ring(C, 1))


def z_ring(block):
    half = block.shape[0] // 2
    ups, downs = [block], [block]
    for _ in range(3):
        ups.append(pz(ups[-1], 1))
        downs.append(pz(downs[-1], -1))
    return ups + downs[1:] + [pz(ups[-1][:half], 1), pz(downs[-1][half:], -1)]


def down_kernel(down_t, out):
    rows = down_t[...].T
    out[...] = jnp.concatenate([rows, jnp.zeros((rows.shape[0], PAD - rows.shape[1]), rows.dtype)], 1)


def place(z, c, off):
    src = lax.rem(z + off + Z, Z)
    return src // 4 ^ c, lax.rem(src, 4)


def first_kernel(*refs):
    blocks, (u4, d4), weights = refs[:7], refs[7:9], refs[9:14]
    keep, send, tok, wts = refs[14:]
    z, xl, c, xh = (lax.axis_index(a) for a in ("z", "xl", "c", "xh"))
    n, units = blocks[0].shape[0], weights[3].shape[1]
    for block, off in zip(blocks, OFFSETS):
        half, at = place(z, c, off)
        tok[pl.ds(pl.multiple_of((half * 4 + at) * n, n), n), :] = block[...]
    half, at = place(z, c, 4)
    for i, part in enumerate((u4, d4)):
        tok[pl.ds(pl.multiple_of((half * 4 + at) * n + i * n // 2, n // 2), n // 2), :] = part[...]
    w, w_m1, w_p1, g2, u2 = weights
    for (gate, up), off in zip(((w.at[0], w.at[1]), (w_m1.at[0], w_m1.at[1]), (w_p1.at[0], w_p1.at[1]), (g2.at[0], u2.at[0])),
                               (0, -1, 1, 2)):
        src = lax.rem(xh * 2 + xl + off + 4, 4)
        dst = (src // 2 ^ xh) * 2 + lax.rem(src, 2)
        wts[dst, :units, :] = gate[...]
        wts[dst, units:, :] = up[...]
    flat = wts[...].reshape(8 * units, wts.shape[2])
    for out, lo in ((send, 4 * n), (keep, 0)):
        out[...] = lax.dot_general(flat, tok[lo:lo + 4 * n, :], (((1,), (1,)), ((), ())),
                                   preferred_element_type=jnp.float32)


def second_kernel(*refs):
    blocks, (u4, d4), near, far = refs[:7], refs[7:9], refs[9], refs[10]
    outs, hid, val = refs[11:15], refs[15], refs[16]
    z, xl, c, y = (lax.axis_index(a) for a in ("z", "xl", "c", "y"))
    n = u4.shape[0]
    rows = 4 * n

    def put(off, part, value):
        half, at = place(z, c, off)
        hid[pl.ds(pl.multiple_of((half * 2 + part) * rows + at * n, 16), n), :] = value

    for block, off in zip(blocks, OFFSETS):
        put(off, 0, block[:n, :])
        put(off, 1, block[n:, :])
    put(4, 0, u4[...])
    put(4, 1, d4[...])
    t = outs[0].shape[0]
    for d in range(2):
        total = None
        for half, down in enumerate((near, far)):
            for h in range(2):
                slot = jnp.where(xl == d, h, 2 + (1 - xl ^ h))
                lo = (half * 2 + h) * rows
                term = lax.dot_general(hid[lo:lo + rows, :], down[slot], (((0,), (0,)), ((), ())),
                                       preferred_element_type=jnp.float32)
                total = term if total is None else total + term
        val[...] = total
        for k, out in enumerate(outs):
            at = lax.rem(y + k, 4) * t
            out[:, d * PAD:(d + 1) * PAD] = val[pl.ds(pl.multiple_of(at, t), t), :].astype(out.dtype)


VMEM = pl.BlockSpec(memory_space=pltpu.VMEM)


def solution(mesh):
    grid = Mesh(mesh.devices.reshape(Z, XL, Y, XH, C), ("z", "xl", "y", "xh", "c"))
    final_axes = ("z", "y", "xh", "c")
    final_perms = ([], [])
    for z in range(Z):
        for y in range(Y):
            for xh in range(XH):
                for c in range(C):
                    src = ((z * Y + y) * XH + xh) * C + c
                    dst = (((4 * c + y) * Y + z // 2) * XH + z % 2) * C
                    final_perms[0].append((src, dst + xh))
                    final_perms[1].append((src, dst + 1 - xh))

    def body(tokens, gate, up, down):
        xh, c = lax.axis_index("xh"), lax.axis_index("c")
        units, k, n = gate.shape[0], tokens.shape[1], tokens.shape[0] // 2
        bf16 = jnp.bfloat16

        toks = z_ring(lax.dynamic_slice_in_dim(tokens, xh * n, n, 0))

        w = jnp.stack([gate, up])
        w_m1, w_p1 = px(w, 1), px(w, -1)
        weights = w, w_m1, w_p1, px(w_m1[:1], 1), px(w_p1[1:], -1)

        dblk = pl.pallas_call(
            down_kernel,
            out_shape=jax.ShapeDtypeStruct((down.shape[0], PAD), bf16),
            in_specs=[VMEM],
            out_specs=VMEM,
            compiler_params=pltpu.CompilerParams(vmem_limit_bytes=4 << 20),
            cost_estimate=pl.CostEstimate(flops=10**8, bytes_accessed=1 << 20, transcendentals=0),
            name="down",
        )(down.T)
        near = jnp.stack([dblk, px(dblk, 2), px(dblk, 1), px(dblk, -1)])
        far = core_swap(near)

        m, t = 8 * units, Z * n
        half = jax.ShapeDtypeStruct((m, t // 2), jnp.float32)
        keep, send = pl.pallas_call(
            first_kernel,
            out_shape=(half, half),
            in_specs=[VMEM] * 14,
            out_specs=(VMEM, VMEM),
            scratch_shapes=[pltpu.VMEM((t, k), bf16), pltpu.VMEM((4, 2 * units, k), bf16)],
            compiler_params=pltpu.CompilerParams(vmem_limit_bytes=12 << 20),
            cost_estimate=pl.CostEstimate(flops=2 * m * t * k, bytes_accessed=2 * k * (m + t), transcendentals=0),
            name="first",
        )(*toks, *weights)
        whole = (keep + core_swap(send)).reshape(4, 2, units, t // 2)
        g, u = whole[:, 0], whole[:, 1]
        hidden = (jax.nn.silu(g) * u).astype(bf16).reshape(4 * units, t // 2)

        hids = z_ring(hidden)
        piece = jax.ShapeDtypeStruct((n, 2 * PAD), bf16)
        shares = pl.pallas_call(
            second_kernel,
            out_shape=(piece,) * 4,
            in_specs=[VMEM] * 11,
            out_specs=(VMEM,) * 4,
            scratch_shapes=[pltpu.VMEM((Z * 4 * units, t // 2), bf16), pltpu.VMEM((t // 2, PAD), jnp.float32)],
            compiler_params=pltpu.CompilerParams(vmem_limit_bytes=10 << 20),
            cost_estimate=pl.CostEstimate(flops=2 * Z * 4 * units * t * PAD, bytes_accessed=6 << 20, transcendentals=0),
            name="second",
        )(*hids, near, far)

        parts = shares[0], py(shares[1], 1), py(shares[2], 2), py(shares[3], -1)
        total = sum(p.astype(jnp.float32) for p in parts).astype(bf16)
        mine, other = (lax.dynamic_slice_in_dim(total, d * PAD, PAD, 1) for d in (xh, 1 - xh))
        got_a, got_b = lax.ppermute(mine, final_axes, final_perms[0]), lax.ppermute(other, final_axes, final_perms[1])
        rows = jnp.where(c == 0, jnp.concatenate([got_a, got_b], 0), jnp.concatenate([got_b, got_a], 0))
        return rows[:, :down.shape[1]]

    row, col = ("z", "xl"), ("y", "xh")
    return jax.shard_map(
        body,
        mesh=grid,
        in_specs=(P(row, "c"), P(col + row, "c"), P(col + row, "c"), P(col + ("c",), row)),
        out_specs=P(row, col + ("c",)),
        check_vma=False,
    )
```

```python
import jax
import jax.numpy as jnp
from jax import lax
from jax.experimental import pallas as pl
from jax.experimental.pallas import tpu as pltpu
from jax.sharding import Mesh, PartitionSpec as P


Z, XL, Y, XH, C = 8, 2, 4, 2, 2
PAD = 384
OFFSETS = (0, -1, -2, -3, 1, 2, 3)


def ring(n, k):
    return [(i, (i + k) % n) for i in range(n)]


def x_ring(k):
    at = [(x % 2) * 2 + x // 2 for x in range(4)]
    return [(at[a], at[b]) for a, b in ring(4, k)]


def px(v, k):
    return lax.ppermute(v, ("xl", "xh"), x_ring(k))


def py(v, k):
    return lax.ppermute(v, "y", ring(Y, k))


def pz(v, k):
    return lax.ppermute(v, "z", ring(Z, k))


def core_swap(v):
    return lax.ppermute(v, "c", ring(C, 1))


def z_ring(block):
    half = block.shape[0] // 2
    ups, downs = [block], [block]
    for _ in range(3):
        ups.append(pz(ups[-1], 1))
        downs.append(pz(downs[-1], -1))
    return ups + downs[1:] + [pz(ups[-1][:half], 1), pz(downs[-1][half:], -1)]


def z_direct(block):
    half = block.shape[0] // 2
    up2, dn2 = pz(block, 2), pz(block, -2)
    up1, dn1 = pz(block, 1), pz(block, -1)
    up4, dn4 = pz(up2[:half], 2), pz(dn2[half:], -2)
    up3, dn3 = pz(up2, 1), pz(dn2, -1)
    return [block, up1, up2, up3, dn1, dn2, dn3, up4, dn4]


def kept(z, c, y):
    def span(a, b, n):
        return min((a - b) % n, (b - a) % n)

    targets = sorted(range(4), key=lambda j: (-span(z, 4 * c + j, Z), j))
    owners = sorted(range(Y), key=lambda w: (span(w, z // 2, Y), w))
    return targets[owners.index(y)]


def kept_at(z, c, y):
    value = jnp.int32(0)
    for cc in range(C):
        for w in range(Y):
            word = sum(kept(zz, cc, w) << (2 * zz) for zz in range(Z))
            value = jnp.where((c == cc) & (y == w), jnp.int32(word), value)
    return lax.shift_right_logical(value, (2 * z).astype(jnp.int32)) & 3


def down_kernel(down_t, out):
    rows = down_t[...].T
    out[...] = jnp.concatenate([rows, jnp.zeros((rows.shape[0], PAD - rows.shape[1]), rows.dtype)], 1)


def place(z, c, off):
    src = lax.rem(z + off + Z, Z)
    return src // 4 ^ c, lax.rem(src, 4)


def first_kernel(*refs):
    blocks, (u4, d4), weights = refs[:7], refs[7:9], refs[9:14]
    keep, send, tok, wts = refs[14:]
    z, xl, c, xh = (lax.axis_index(a) for a in ("z", "xl", "c", "xh"))
    n, units = blocks[0].shape[0], weights[3].shape[1]
    for block, off in zip(blocks, OFFSETS):
        half, at = place(z, c, off)
        tok[pl.ds(pl.multiple_of((half * 4 + at) * n, n), n), :] = block[...]
    half, at = place(z, c, 4)
    for i, part in enumerate((u4, d4)):
        tok[pl.ds(pl.multiple_of((half * 4 + at) * n + i * n // 2, n // 2), n // 2), :] = part[...]
    w, w_m1, w_p1, g2, u2 = weights
    for (gate, up), off in zip(((w.at[0], w.at[1]), (w_m1.at[0], w_m1.at[1]), (w_p1.at[0], w_p1.at[1]), (g2.at[0], u2.at[0])),
                               (0, -1, 1, 2)):
        src = lax.rem(xh * 2 + xl + off + 4, 4)
        dst = (src // 2 ^ xh) * 2 + lax.rem(src, 2)
        wts[dst, :units, :] = gate[...]
        wts[dst, units:, :] = up[...]
    flat = wts[...].reshape(8 * units, wts.shape[2])
    for out, lo in ((send, 4 * n), (keep, 0)):
        out[...] = lax.dot_general(flat, tok[lo:lo + 4 * n, :], (((1,), (1,)), ((), ())),
                                   preferred_element_type=jnp.float32)


def second_kernel(*refs):
    blocks, (u4, d4), near, far = refs[:7], refs[7:9], refs[9], refs[10]
    outs, hid, val = refs[11:15], refs[15], refs[16]
    z, xl, c, y = (lax.axis_index(a) for a in ("z", "xl", "c", "y"))
    n = u4.shape[0]
    rows = 4 * n

    def put(off, part, value):
        half, at = place(z, c, off)
        hid[pl.ds(pl.multiple_of((half * 2 + part) * rows + at * n, 16), n), :] = value

    for block, off in zip(blocks, OFFSETS):
        put(off, 0, block[:n, :])
        put(off, 1, block[n:, :])
    put(4, 0, u4[...])
    put(4, 1, d4[...])
    t = outs[0].shape[0]
    for d in range(2):
        total = None
        for half, down in enumerate((near, far)):
            for h in range(2):
                slot = jnp.where(xl == d, h, 2 + (1 - xl ^ h))
                lo = (half * 2 + h) * rows
                term = lax.dot_general(hid[lo:lo + rows, :], down[slot], (((0,), (0,)), ((), ())),
                                       preferred_element_type=jnp.float32)
                total = term if total is None else total + term
        val[...] = total
        for k, out in enumerate(outs):
            at = kept_at(z, c, lax.rem(y + k, 4)) * t
            out[:, d * PAD:(d + 1) * PAD] = val[pl.ds(pl.multiple_of(at, t), t), :].astype(out.dtype)


VMEM = pl.BlockSpec(memory_space=pltpu.VMEM)


def solution(mesh):
    grid = Mesh(mesh.devices.reshape(Z, XL, Y, XH, C), ("z", "xl", "y", "xh", "c"))
    final_axes = ("z", "y", "xh", "c")
    final_perms = ([], [])
    for z in range(Z):
        for y in range(Y):
            for xh in range(XH):
                for c in range(C):
                    src = ((z * Y + y) * XH + xh) * C + c
                    dst = (((4 * c + kept(z, c, y)) * Y + z // 2) * XH + z % 2) * C
                    final_perms[0].append((src, dst + xh))
                    final_perms[1].append((src, dst + 1 - xh))

    def body(tokens, gate, up, down):
        xh, c = lax.axis_index("xh"), lax.axis_index("c")
        units, k, n = gate.shape[0], tokens.shape[1], tokens.shape[0] // 2
        bf16 = jnp.bfloat16

        toks = z_ring(lax.dynamic_slice_in_dim(tokens, xh * n, n, 0))

        w = jnp.stack([gate, up])
        w_m1, w_p1 = px(w, 1), px(w, -1)
        weights = w, w_m1, w_p1, px(w_m1[:1], 1), px(w_p1[1:], -1)

        dblk = pl.pallas_call(
            down_kernel,
            out_shape=jax.ShapeDtypeStruct((down.shape[0], PAD), bf16),
            in_specs=[VMEM],
            out_specs=VMEM,
            compiler_params=pltpu.CompilerParams(vmem_limit_bytes=4 << 20),
            cost_estimate=pl.CostEstimate(flops=10**8, bytes_accessed=1 << 20, transcendentals=0),
            name="down",
        )(down.T)
        near = [dblk, px(dblk, 2), px(dblk, 1), px(dblk, -1)]
        near = jnp.stack(near)
        far = core_swap(near)

        m, t = 8 * units, Z * n
        half = jax.ShapeDtypeStruct((m, t // 2), jnp.float32)
        keep, send = pl.pallas_call(
            first_kernel,
            out_shape=(half, half),
            in_specs=[VMEM] * 14,
            out_specs=(VMEM, VMEM),
            scratch_shapes=[pltpu.VMEM((t, k), bf16), pltpu.VMEM((4, 2 * units, k), bf16)],
            compiler_params=pltpu.CompilerParams(vmem_limit_bytes=12 << 20),
            cost_estimate=pl.CostEstimate(flops=2 * m * t * k, bytes_accessed=2 * k * (m + t), transcendentals=0),
            name="first",
        )(*toks, *weights)
        whole = (keep + core_swap(send)).reshape(4, 2, units, t // 2)
        g, u = whole[:, 0], whole[:, 1]
        hidden = (jax.nn.silu(g) * u).astype(bf16).reshape(4 * units, t // 2)

        hids = z_direct(hidden)
        piece = jax.ShapeDtypeStruct((n, 2 * PAD), bf16)
        shares = pl.pallas_call(
            second_kernel,
            out_shape=(piece,) * 4,
            in_specs=[VMEM] * 11,
            out_specs=(VMEM,) * 4,
            scratch_shapes=[pltpu.VMEM((Z * 4 * units, t // 2), bf16), pltpu.VMEM((t // 2, PAD), jnp.float32)],
            compiler_params=pltpu.CompilerParams(vmem_limit_bytes=10 << 20),
            cost_estimate=pl.CostEstimate(flops=2 * Z * 4 * units * t * PAD, bytes_accessed=6 << 20, transcendentals=0),
            name="second",
        )(*hids, near, far)

        parts = shares[0], py(shares[1], 1), py(shares[2], 2), py(shares[3], -1)
        total = sum(p.astype(jnp.float32) for p in parts).astype(bf16)
        mine, other = (lax.dynamic_slice_in_dim(total, d * PAD, PAD, 1) for d in (xh, 1 - xh))
        got_a, got_b = lax.ppermute(mine, final_axes, final_perms[0]), lax.ppermute(other, final_axes, final_perms[1])
        rows = jnp.where(c == 0, jnp.concatenate([got_a, got_b], 0), jnp.concatenate([got_b, got_a], 0))
        return rows[:, :down.shape[1]]

    row, col = ("z", "xl"), ("y", "xh")
    return jax.shard_map(
        body,
        mesh=grid,
        in_specs=(P(row, "c"), P(col + row, "c"), P(col + row, "c"), P(col + ("c",), row)),
        out_specs=P(row, col + ("c",)),
        check_vma=False,
    )
```

```python
import jax
import jax.numpy as jnp
from jax import lax
from jax.experimental import pallas as pl
from jax.experimental.pallas import tpu as pltpu
from jax.sharding import Mesh, PartitionSpec as P


Z, XL, Y, XH, C = 8, 2, 4, 2, 2
PAD = 384
OFFSETS = (0, -1, -2, -3, 1, 2, 3)


def ring(n, k):
    return [(i, (i + k) % n) for i in range(n)]


def x_ring(k):
    at = [(x % 2) * 2 + x // 2 for x in range(4)]
    return [(at[a], at[b]) for a, b in ring(4, k)]


def px(v, k):
    return lax.ppermute(v, ("xl", "xh"), x_ring(k))


def py(v, k):
    return lax.ppermute(v, "y", ring(Y, k))


def pz(v, k):
    return lax.ppermute(v, "z", ring(Z, k))


def core_swap(v):
    return lax.ppermute(v, "c", ring(C, 1))


def z_ring(block):
    half = block.shape[0] // 2
    ups, downs = [block], [block]
    for _ in range(3):
        ups.append(pz(ups[-1], 1))
        downs.append(pz(downs[-1], -1))
    return ups + downs[1:] + [pz(ups[-1][:half], 1), pz(downs[-1][half:], -1)]


def z_direct(block):
    half = block.shape[0] // 2
    up2, dn2 = pz(block, 2), pz(block, -2)
    up1, dn1 = pz(block, 1), pz(block, -1)
    up4, dn4 = pz(up2[:half], 2), pz(dn2[half:], -2)
    up3, dn3 = pz(up2, 1), pz(dn2, -1)
    return [block, up1, up2, up3, dn1, dn2, dn3, up4, dn4]


def kept(z, c, y):
    def span(a, b, n):
        return min((a - b) % n, (b - a) % n)

    targets = sorted(range(4), key=lambda j: (-span(z, 4 * c + j, Z), j))
    owners = sorted(range(Y), key=lambda w: (span(w, z // 2, Y), w))
    return targets[owners.index(y)]


def kept_at(z, c, y):
    value = jnp.int32(0)
    for cc in range(C):
        for w in range(Y):
            word = sum(kept(zz, cc, w) << (2 * zz) for zz in range(Z))
            value = jnp.where((c == cc) & (y == w), jnp.int32(word), value)
    return lax.shift_right_logical(value, (2 * z).astype(jnp.int32)) & 3


def down_kernel(down_t, out):
    rows = down_t[...].T
    out[...] = jnp.concatenate([rows, jnp.zeros((rows.shape[0], PAD - rows.shape[1]), rows.dtype)], 1)


def place(z, c, off):
    src = lax.rem(z + off + Z, Z)
    return src // 4 ^ c, lax.rem(src, 4)


def first_kernel(*refs):
    blocks, (u4, d4), weights = refs[:7], refs[7:9], refs[9:14]
    send, tok, wts, far_tok = refs[14:]
    z, xl, c, xh = (lax.axis_index(a) for a in ("z", "xl", "c", "xh"))
    n, units = blocks[0].shape[0], weights[3].shape[1]

    def put(off, lo, rows):
        half, at = place(z, c, off)
        at = pl.multiple_of(at * n + lo, n // 2)

        @pl.when(half == 0)
        def _():
            tok[pl.ds(at, rows.shape[0]), :] = rows[...]

        @pl.when(half != 0)
        def _():
            far_tok[pl.ds(at, rows.shape[0]), :] = rows[...]

    for block, off in zip(blocks, OFFSETS):
        put(off, 0, block)
    for i, part in enumerate((u4, d4)):
        put(4, i * n // 2, part)
    w, w_m1, w_p1, g2, u2 = weights
    for (gate, up), off in zip(((w.at[0], w.at[1]), (w_m1.at[0], w_m1.at[1]), (w_p1.at[0], w_p1.at[1]), (g2.at[0], u2.at[0])),
                               (0, -1, 1, 2)):
        src = lax.rem(xh * 2 + xl + off + 4, 4)
        dst = (src // 2 ^ xh) * 2 + lax.rem(src, 2)
        wts[dst, :units, :] = gate[...]
        wts[dst, units:, :] = up[...]
    half_product(far_tok, wts, send)


def half_product(tok, wts, out):
    flat = wts[...].reshape(out.shape[0], wts.shape[2])
    out[...] = lax.dot_general(flat, tok[...], (((1,), (1,)), ((), ())), preferred_element_type=jnp.float32)


def second_kernel(*refs):
    blocks, (u4, d4), near, far = refs[:7], refs[7:9], refs[9], refs[10]
    outs, hid, val = refs[11:15], refs[15], refs[16]
    z, xl, c, y = (lax.axis_index(a) for a in ("z", "xl", "c", "y"))
    n = u4.shape[0]
    rows = 4 * n

    def put(off, part, value):
        half, at = place(z, c, off)
        hid[pl.ds(pl.multiple_of((half * 2 + part) * rows + at * n, 16), n), :] = value

    for block, off in zip(blocks, OFFSETS):
        put(off, 0, block[:n, :])
        put(off, 1, block[n:, :])
    put(4, 0, u4[...])
    put(4, 1, d4[...])
    t = outs[0].shape[0]
    for d in range(2):
        total = None
        for half, down in enumerate((near, far)):
            for h in range(2):
                slot = jnp.where(xl == d, h, 2 + (1 - xl ^ h))
                lo = (half * 2 + h) * rows
                term = lax.dot_general(hid[lo:lo + rows, :], down[slot], (((0,), (0,)), ((), ())),
                                       preferred_element_type=jnp.float32)
                total = term if total is None else total + term
        val[...] = total
        for k, out in enumerate(outs):
            at = kept_at(z, c, lax.rem(y + k, 4)) * t
            out[:, d * PAD:(d + 1) * PAD] = val[pl.ds(pl.multiple_of(at, t), t), :].astype(out.dtype)


VMEM = pl.BlockSpec(memory_space=pltpu.VMEM)


def solution(mesh):
    grid = Mesh(mesh.devices.reshape(Z, XL, Y, XH, C), ("z", "xl", "y", "xh", "c"))
    final_axes = ("z", "y", "xh", "c")
    final_perms = ([], [])
    for z in range(Z):
        for y in range(Y):
            for xh in range(XH):
                for c in range(C):
                    src = ((z * Y + y) * XH + xh) * C + c
                    dst = (((4 * c + kept(z, c, y)) * Y + z // 2) * XH + z % 2) * C
                    final_perms[0].append((src, dst + xh))
                    final_perms[1].append((src, dst + 1 - xh))

    def body(tokens, gate, up, down):
        xh, c = lax.axis_index("xh"), lax.axis_index("c")
        units, k, n = gate.shape[0], tokens.shape[1], tokens.shape[0] // 2
        bf16 = jnp.bfloat16

        toks = z_ring(lax.dynamic_slice_in_dim(tokens, xh * n, n, 0))

        w = jnp.stack([gate, up])
        w_m1, w_p1 = px(w, 1), px(w, -1)
        weights = w, w_m1, w_p1, px(w_m1[:1], 1), px(w_p1[1:], -1)

        dblk = pl.pallas_call(
            down_kernel,
            out_shape=jax.ShapeDtypeStruct((down.shape[0], PAD), bf16),
            in_specs=[VMEM],
            out_specs=VMEM,
            compiler_params=pltpu.CompilerParams(vmem_limit_bytes=4 << 20),
            cost_estimate=pl.CostEstimate(flops=10**8, bytes_accessed=1 << 20, transcendentals=0),
            name="down",
        )(down.T)
        near = [dblk, px(dblk, 2), px(dblk, 1), px(dblk, -1)]
        near = jnp.stack(near)
        far = core_swap(near)

        m, t = 8 * units, Z * n
        half = jax.ShapeDtypeStruct((m, t // 2), jnp.float32)
        send, tok, wts = pl.pallas_call(
            first_kernel,
            out_shape=(half, jax.ShapeDtypeStruct((t // 2, k), bf16), jax.ShapeDtypeStruct((4, 2 * units, k), bf16)),
            in_specs=[VMEM] * 14,
            out_specs=(VMEM,) * 3,
            scratch_shapes=[pltpu.VMEM((t // 2, k), bf16)],
            compiler_params=pltpu.CompilerParams(vmem_limit_bytes=12 << 20),
            cost_estimate=pl.CostEstimate(flops=m * t * k, bytes_accessed=2 * k * (m + t), transcendentals=0),
            name="first",
        )(*toks, *weights)
        keep = pl.pallas_call(
            half_product,
            out_shape=half,
            in_specs=[VMEM] * 2,
            out_specs=VMEM,
            compiler_params=pltpu.CompilerParams(vmem_limit_bytes=8 << 20),
            cost_estimate=pl.CostEstimate(flops=m * t * k, bytes_accessed=2 * k * (m + t), transcendentals=0),
            name="keep",
        )(tok, wts)
        whole = (keep + core_swap(send)).reshape(4, 2, units, t // 2)
        g, u = whole[:, 0], whole[:, 1]
        hidden = (jax.nn.silu(g) * u).astype(bf16).reshape(4 * units, t // 2)

        hids = z_direct(hidden)
        piece = jax.ShapeDtypeStruct((n, 2 * PAD), bf16)
        shares = pl.pallas_call(
            second_kernel,
            out_shape=(piece,) * 4,
            in_specs=[VMEM] * 11,
            out_specs=(VMEM,) * 4,
            scratch_shapes=[pltpu.VMEM((Z * 4 * units, t // 2), bf16), pltpu.VMEM((t // 2, PAD), jnp.float32)],
            compiler_params=pltpu.CompilerParams(vmem_limit_bytes=10 << 20),
            cost_estimate=pl.CostEstimate(flops=2 * Z * 4 * units * t * PAD, bytes_accessed=6 << 20, transcendentals=0),
            name="second",
        )(*hids, near, far)

        parts = shares[0], py(shares[1], 1), py(shares[2], 2), py(shares[3], -1)
        total = sum(p.astype(jnp.float32) for p in parts).astype(bf16)
        mine, other = (lax.dynamic_slice_in_dim(total, d * PAD, PAD, 1) for d in (xh, 1 - xh))
        got_a, got_b = lax.ppermute(mine, final_axes, final_perms[0]), lax.ppermute(other, final_axes, final_perms[1])
        rows = jnp.where(c == 0, jnp.concatenate([got_a, got_b], 0), jnp.concatenate([got_b, got_a], 0))
        return rows[:, :down.shape[1]]

    row, col = ("z", "xl"), ("y", "xh")
    return jax.shard_map(
        body,
        mesh=grid,
        in_specs=(P(row, "c"), P(col + row, "c"), P(col + row, "c"), P(col + ("c",), row)),
        out_specs=P(row, col + ("c",)),
        check_vma=False,
    )
```

```python
import jax
import jax.numpy as jnp
from jax import lax
from jax.experimental import pallas as pl
from jax.experimental.pallas import tpu as pltpu
from jax.sharding import Mesh, PartitionSpec as P


Z, XL, Y, XH, C = 8, 2, 4, 2, 2
PAD = 384
OFFSETS = (0, -1, -2, -3, 1, 2, 3)


def ring(n, k):
    return [(i, (i + k) % n) for i in range(n)]


def x_ring(k):
    at = [(x % 2) * 2 + x // 2 for x in range(4)]
    return [(at[a], at[b]) for a, b in ring(4, k)]


def px(v, k):
    return lax.ppermute(v, ("xl", "xh"), x_ring(k))


def py(v, k):
    return lax.ppermute(v, "y", ring(Y, k))


def pz(v, k):
    return lax.ppermute(v, "z", ring(Z, k))


def core_swap(v):
    return lax.ppermute(v, "c", ring(C, 1))


def z_ring(block):
    half = block.shape[0] // 2
    ups, downs = [block], [block]
    for _ in range(3):
        ups.append(pz(ups[-1], 1))
        downs.append(pz(downs[-1], -1))
    return ups + downs[1:] + [pz(ups[-1][:half], 1), pz(downs[-1][half:], -1)]


def z_direct(block):
    half = block.shape[0] // 2
    up2, dn2 = pz(block, 2), pz(block, -2)
    up1, dn1 = pz(block, 1), pz(block, -1)
    up4, dn4 = pz(up2[:half], 2), pz(dn2[half:], -2)
    up3, dn3 = pz(up2, 1), pz(dn2, -1)
    return [block, up1, up2, up3, dn1, dn2, dn3, up4, dn4]


def kept(z, c, y):
    def span(a, b, n):
        return min((a - b) % n, (b - a) % n)

    targets = sorted(range(4), key=lambda j: (-span(z, 4 * c + j, Z), j))
    owners = sorted(range(Y), key=lambda w: (span(w, z // 2, Y), w))
    return targets[owners.index(y)]


def kept_at(z, c, y):
    value = jnp.int32(0)
    for cc in range(C):
        for w in range(Y):
            word = sum(kept(zz, cc, w) << (2 * zz) for zz in range(Z))
            value = jnp.where((c == cc) & (y == w), jnp.int32(word), value)
    return lax.shift_right_logical(value, (2 * z).astype(jnp.int32)) & 3


def down_kernel(down_t, out):
    rows = down_t[...].T
    out[...] = jnp.concatenate([rows, jnp.zeros((rows.shape[0], PAD - rows.shape[1]), rows.dtype)], 1)


def place(z, c, off):
    src = lax.rem(z + off + Z, Z)
    return src // 4 ^ c, lax.rem(src, 4)


def first_kernel(*refs):
    blocks, (u4, d4), weights = refs[:7], refs[7:9], refs[9:14]
    send, tok, wts, far_tok = refs[14:]
    z, xl, c, xh = (lax.axis_index(a) for a in ("z", "xl", "c", "xh"))
    n, units = blocks[0].shape[0], weights[3].shape[1]

    def put(off, lo, rows):
        half, at = place(z, c, off)
        at = pl.multiple_of(at * n + lo, n // 2)

        @pl.when(half == 0)
        def _():
            tok[pl.ds(at, rows.shape[0]), :] = rows[...]

        @pl.when(half != 0)
        def _():
            far_tok[pl.ds(at, rows.shape[0]), :] = rows[...]

    for block, off in zip(blocks, OFFSETS):
        put(off, 0, block)
    for i, part in enumerate((u4, d4)):
        put(4, i * n // 2, part)
    w, w_m1, w_p1, g2, u2 = weights
    for (gate, up), off in zip(((w.at[0], w.at[1]), (w_m1.at[0], w_m1.at[1]), (w_p1.at[0], w_p1.at[1]), (g2.at[0], u2.at[0])),
                               (0, -1, 1, 2)):
        src = lax.rem(xh * 2 + xl + off + 4, 4)
        dst = (src // 2 ^ xh) * 2 + lax.rem(src, 2)
        wts[dst, :units, :] = gate[...]
        wts[dst, units:, :] = up[...]
    half_product(far_tok, wts, send)


def out_kernel(a, b, out):
    c, f = lax.axis_index("c"), out.shape[0]
    rows = jnp.concatenate([jnp.where(c == 0, a[...], b[...]), jnp.where(c == 0, b[...], a[...])], 0)
    out[...] = rows.T[:f, :]


def half_product(tok, wts, out):
    flat = wts[...].reshape(out.shape[0], wts.shape[2])
    out[...] = lax.dot_general(flat, tok[...], (((1,), (1,)), ((), ())), preferred_element_type=jnp.float32)


def second_kernel(*refs):
    blocks, (u4, d4), near, far = refs[:7], refs[7:9], refs[9], refs[10]
    outs, hid, val = refs[11:15], refs[15], refs[16]
    z, xl, c, y = (lax.axis_index(a) for a in ("z", "xl", "c", "y"))
    n = u4.shape[0]
    rows = 4 * n

    def put(off, part, value):
        half, at = place(z, c, off)
        hid[pl.ds(pl.multiple_of((half * 2 + part) * rows + at * n, 16), n), :] = value

    for block, off in zip(blocks, OFFSETS):
        put(off, 0, block[:n, :])
        put(off, 1, block[n:, :])
    put(4, 0, u4[...])
    put(4, 1, d4[...])
    t, k = outs[0].shape[0], 2 * rows
    dims = (((0,), (0,)), ((), ()))
    val[...] = lax.dot_general(hid[:k, :], near[...], dims, preferred_element_type=jnp.float32)
    val[...] += lax.dot_general(hid[k:, :], far[...], dims, preferred_element_type=jnp.float32)
    for i, out in enumerate(outs):
        at = pl.multiple_of(kept_at(z, c, lax.rem(y + i, 4)) * t, t)
        for f in range(2):
            out[:, pl.ds(pl.multiple_of((f ^ xl) * PAD, PAD), PAD)] = val[pl.ds(at, t), f * PAD:(f + 1) * PAD].astype(out.dtype)


VMEM = pl.BlockSpec(memory_space=pltpu.VMEM)


def solution(mesh):
    grid = Mesh(mesh.devices.reshape(Z, XL, Y, XH, C), ("z", "xl", "y", "xh", "c"))
    final_axes = ("z", "y", "xh", "c")
    final_perms = ([], [])
    for z in range(Z):
        for y in range(Y):
            for xh in range(XH):
                for c in range(C):
                    src = ((z * Y + y) * XH + xh) * C + c
                    dst = (((4 * c + kept(z, c, y)) * Y + z // 2) * XH + z % 2) * C
                    final_perms[0].append((src, dst + xh))
                    final_perms[1].append((src, dst + 1 - xh))

    def body(tokens, gate, up, down):
        xl, xh, _ = (lax.axis_index(a) for a in ("xl", "xh", "c"))
        units, k, n = gate.shape[0], tokens.shape[1], tokens.shape[0] // 2
        bf16 = jnp.bfloat16

        toks = z_ring(lax.dynamic_slice_in_dim(tokens, xh * n, n, 0))

        w = jnp.stack([gate, up])
        w_m1, w_p1 = px(w, 1), px(w, -1)
        weights = w, w_m1, w_p1, px(w_m1[:1], 1), px(w_p1[1:], -1)

        dblk = pl.pallas_call(
            down_kernel,
            out_shape=jax.ShapeDtypeStruct((down.shape[0], PAD), bf16),
            in_specs=[VMEM],
            out_specs=VMEM,
            compiler_params=pltpu.CompilerParams(vmem_limit_bytes=4 << 20),
            cost_estimate=pl.CostEstimate(flops=10**8, bytes_accessed=1 << 20, transcendentals=0),
            name="down",
        )(down.T)
        d_2, d_m1, d_p1 = px(dblk, 2), px(dblk, 1), px(dblk, -1)
        same, other = jnp.where(xl == 0, d_p1, d_m1), jnp.where(xl == 0, d_m1, d_p1)
        near = jnp.concatenate([jnp.concatenate([dblk, same], 1), jnp.concatenate([d_2, other], 1)], 0)
        far = core_swap(near)

        m, t = 8 * units, Z * n
        half = jax.ShapeDtypeStruct((m, t // 2), jnp.float32)
        send, tok, wts = pl.pallas_call(
            first_kernel,
            out_shape=(half, jax.ShapeDtypeStruct((t // 2, k), bf16), jax.ShapeDtypeStruct((4, 2 * units, k), bf16)),
            in_specs=[VMEM] * 14,
            out_specs=(VMEM,) * 3,
            scratch_shapes=[pltpu.VMEM((t // 2, k), bf16)],
            compiler_params=pltpu.CompilerParams(vmem_limit_bytes=12 << 20),
            cost_estimate=pl.CostEstimate(flops=m * t * k, bytes_accessed=2 * k * (m + t), transcendentals=0),
            name="first",
        )(*toks, *weights)
        keep = pl.pallas_call(
            half_product,
            out_shape=half,
            in_specs=[VMEM] * 2,
            out_specs=VMEM,
            compiler_params=pltpu.CompilerParams(vmem_limit_bytes=8 << 20),
            cost_estimate=pl.CostEstimate(flops=m * t * k, bytes_accessed=2 * k * (m + t), transcendentals=0),
            name="keep",
        )(tok, wts)
        whole = (keep + core_swap(send)).reshape(4, 2, units, t // 2)
        g, u = whole[:, 0], whole[:, 1]
        hidden = (jax.nn.silu(g) * u).astype(bf16).reshape(4 * units, t // 2)

        hids = z_direct(hidden)
        piece = jax.ShapeDtypeStruct((n, 2 * PAD), bf16)
        shares = pl.pallas_call(
            second_kernel,
            out_shape=(piece,) * 4,
            in_specs=[VMEM] * 11,
            out_specs=(VMEM,) * 4,
            scratch_shapes=[pltpu.VMEM((Z * 4 * units, t // 2), bf16), pltpu.VMEM((t // 2, 2 * PAD), jnp.float32)],
            compiler_params=pltpu.CompilerParams(vmem_limit_bytes=10 << 20),
            cost_estimate=pl.CostEstimate(flops=2 * Z * 4 * units * t * PAD, bytes_accessed=6 << 20, transcendentals=0),
            name="second",
        )(*hids, near, far)

        parts = shares[0], py(shares[1], 1), py(shares[2], 2), py(shares[3], -1)
        total = sum(p.astype(jnp.float32) for p in parts).astype(bf16)
        mine, other = (lax.dynamic_slice_in_dim(total, d * PAD, PAD, 1) for d in (xh, 1 - xh))
        got_a, got_b = lax.ppermute(mine, final_axes, final_perms[0]), lax.ppermute(other, final_axes, final_perms[1])
        return pl.pallas_call(
            out_kernel,
            out_shape=jax.ShapeDtypeStruct((down.shape[1], 2 * n), bf16),
            in_specs=[VMEM] * 2,
            out_specs=VMEM,
            compiler_params=pltpu.CompilerParams(vmem_limit_bytes=4 << 20),
            name="out",
        )(got_a, got_b).T

    row, col = ("z", "xl"), ("y", "xh")
    return jax.shard_map(
        body,
        mesh=grid,
        in_specs=(P(row, "c"), P(col + row, "c"), P(col + row, "c"), P(col + ("c",), row)),
        out_specs=P(row, col + ("c",)),
        check_vma=False,
    )
```

```python
import jax
import jax.numpy as jnp
from jax import lax
from jax.experimental import pallas as pl
from jax.experimental.pallas import tpu as pltpu
from jax.sharding import Mesh, PartitionSpec as P


Z, XL, Y, XH, C = 8, 2, 4, 2, 2
PAD = 384
OFFSETS = (0, -1, -2, -3, 1, 2, 3)


def ring(n, k):
    return [(i, (i + k) % n) for i in range(n)]


def x_ring(k):
    at = [(x % 2) * 2 + x // 2 for x in range(4)]
    return [(at[a], at[b]) for a, b in ring(4, k)]


def px(v, k):
    return lax.ppermute(v, ("xl", "xh"), x_ring(k))


def py(v, k):
    return lax.ppermute(v, "y", ring(Y, k))


def pz(v, k):
    return lax.ppermute(v, "z", ring(Z, k))


def core_swap(v):
    return lax.ppermute(v, "c", ring(C, 1))


def z_ring(block):
    half = block.shape[0] // 2
    ups, downs = [block], [block]
    for _ in range(3):
        ups.append(pz(ups[-1], 1))
        downs.append(pz(downs[-1], -1))
    return ups + downs[1:] + [pz(ups[-1][:half], 1), pz(downs[-1][half:], -1)]


def z_direct(block):
    half = block.shape[0] // 2
    up2, dn2 = pz(block, 2), pz(block, -2)
    up1, dn1 = pz(block, 1), pz(block, -1)
    up4, dn4 = pz(up2[:half], 2), pz(dn2[half:], -2)
    up3, dn3 = pz(up2, 1), pz(dn2, -1)
    return [block, up1, up2, up3, dn1, dn2, dn3, up4, dn4]


def kept(z, c, y):
    def span(a, b, n):
        return min((a - b) % n, (b - a) % n)

    targets = sorted(range(4), key=lambda j: (-span(z, 4 * c + j, Z), j))
    owners = sorted(range(Y), key=lambda w: (span(w, z // 2, Y), w))
    return targets[owners.index(y)]


def kept_at(z, c, y):
    value = jnp.int32(0)
    for cc in range(C):
        for w in range(Y):
            word = sum(kept(zz, cc, w) << (2 * zz) for zz in range(Z))
            value = jnp.where((c == cc) & (y == w), jnp.int32(word), value)
    return lax.shift_right_logical(value, (2 * z).astype(jnp.int32)) & 3


def down_kernel(down_t, out):
    rows = down_t[...].T
    out[...] = jnp.concatenate([rows, jnp.zeros((rows.shape[0], PAD - rows.shape[1]), rows.dtype)], 1)


def place(z, c, off):
    src = lax.rem(z + off + Z, Z)
    return src // 4 ^ c, lax.rem(src, 4)


def write_rows(near, far, off, lo, rows):
    n = near.shape[0] // 4
    half, at = place(lax.axis_index("z"), lax.axis_index("c"), off)
    at = pl.multiple_of(at * n + lo, n // 2)
    for which, dst in enumerate((near, far)):
        @pl.when(half == which)
        def _():
            dst[pl.ds(at, rows.shape[0]), :] = rows[...]


def unit_slot(off):
    xl, xh = lax.axis_index("xl"), lax.axis_index("xh")
    src = lax.rem(xh * 2 + xl + off + 4, 4)
    return (src // 2 ^ xh) * 2 + lax.rem(src, 2)


def gather_kernel(*refs):
    blocks, weights, (near, far, wts) = refs[:7], refs[7:10], refs[10:]
    units = weights[0].shape[1]
    for block, off in zip(blocks, OFFSETS):
        write_rows(near, far, off, 0, block)
    for w, off in zip(weights, (0, -1, 1)):
        for i in range(2):
            wts[unit_slot(off), i * units:(i + 1) * units, :] = w[i]


def first_kernel(u4, d4, gate, up, near_in, far_in, wts_in, send, near, far, wts):
    units = gate.shape[1]
    for i, rows in enumerate((u4, d4)):
        write_rows(near, far, 4, i * rows.shape[0], rows)
    for i, w in enumerate((gate, up)):
        wts[unit_slot(2), i * units:(i + 1) * units, :] = w[0]
    half_product(far, wts, send)


def out_kernel(a, b, out):
    c, f = lax.axis_index("c"), out.shape[0]
    rows = jnp.concatenate([jnp.where(c == 0, a[...], b[...]), jnp.where(c == 0, b[...], a[...])], 0)
    out[...] = rows.T[:f, :]


def half_product(tok, wts, out):
    flat = wts[...].reshape(out.shape[0], wts.shape[2])
    out[...] = lax.dot_general(flat, tok[...], (((1,), (1,)), ((), ())), preferred_element_type=jnp.float32)


def second_kernel(*refs):
    blocks, (u4, d4), near, far = refs[:7], refs[7:9], refs[9], refs[10]
    outs, hid, val = refs[11:15], refs[15], refs[16]
    z, xl, c, y = (lax.axis_index(a) for a in ("z", "xl", "c", "y"))
    n = u4.shape[0]
    rows = 4 * n

    def put(off, part, value):
        half, at = place(z, c, off)
        hid[pl.ds(pl.multiple_of((half * 2 + part) * rows + at * n, 16), n), :] = value

    for block, off in zip(blocks, OFFSETS):
        put(off, 0, block[:n, :])
        put(off, 1, block[n:, :])
    put(4, 0, u4[...])
    put(4, 1, d4[...])
    t, k = outs[0].shape[0], 2 * rows
    dims = (((0,), (0,)), ((), ()))
    val[...] = lax.dot_general(hid[:k, :], near[...], dims, preferred_element_type=jnp.float32)
    val[...] += lax.dot_general(hid[k:, :], far[...], dims, preferred_element_type=jnp.float32)
    for i, out in enumerate(outs):
        at = pl.multiple_of(kept_at(z, c, lax.rem(y + i, 4)) * t, t)
        for f in range(2):
            out[:, pl.ds(pl.multiple_of((f ^ xl) * PAD, PAD), PAD)] = val[pl.ds(at, t), f * PAD:(f + 1) * PAD].astype(out.dtype)


VMEM = pl.BlockSpec(memory_space=pltpu.VMEM)


def solution(mesh):
    grid = Mesh(mesh.devices.reshape(Z, XL, Y, XH, C), ("z", "xl", "y", "xh", "c"))
    final_axes = ("z", "y", "xh", "c")
    final_perms = ([], [])
    for z in range(Z):
        for y in range(Y):
            for xh in range(XH):
                for c in range(C):
                    src = ((z * Y + y) * XH + xh) * C + c
                    dst = (((4 * c + kept(z, c, y)) * Y + z // 2) * XH + z % 2) * C
                    final_perms[0].append((src, dst + xh))
                    final_perms[1].append((src, dst + 1 - xh))

    def body(tokens, gate, up, down):
        xl, xh, _ = (lax.axis_index(a) for a in ("xl", "xh", "c"))
        units, k, n = gate.shape[0], tokens.shape[1], tokens.shape[0] // 2
        bf16 = jnp.bfloat16

        toks = z_ring(lax.dynamic_slice_in_dim(tokens, xh * n, n, 0))

        w = jnp.stack([gate, up])
        w_m1, w_p1 = px(w, 1), px(w, -1)
        weights = w, w_m1, w_p1, px(w_m1[:1], 1), px(w_p1[1:], -1)

        dblk = pl.pallas_call(
            down_kernel,
            out_shape=jax.ShapeDtypeStruct((down.shape[0], PAD), bf16),
            in_specs=[VMEM],
            out_specs=VMEM,
            compiler_params=pltpu.CompilerParams(vmem_limit_bytes=4 << 20),
            cost_estimate=pl.CostEstimate(flops=10**8, bytes_accessed=1 << 20, transcendentals=0),
            name="down",
        )(down.T)
        d_2, d_m1, d_p1 = px(dblk, 2), px(dblk, 1), px(dblk, -1)
        same, other = jnp.where(xl == 0, d_p1, d_m1), jnp.where(xl == 0, d_m1, d_p1)
        near = jnp.concatenate([jnp.concatenate([dblk, same], 1), jnp.concatenate([d_2, other], 1)], 0)
        far = core_swap(near)

        m, t = 8 * units, Z * n
        half = jax.ShapeDtypeStruct((m, t // 2), jnp.float32)
        token_half, blocks = jax.ShapeDtypeStruct((t // 2, k), bf16), jax.ShapeDtypeStruct((4, 2 * units, k), bf16)
        placed = pl.pallas_call(
            gather_kernel,
            out_shape=(token_half, token_half, blocks),
            in_specs=[VMEM] * 10,
            out_specs=(VMEM,) * 3,
            compiler_params=pltpu.CompilerParams(vmem_limit_bytes=4 << 20),
            cost_estimate=pl.CostEstimate(flops=10**8, bytes_accessed=6 << 20, transcendentals=0),
            name="gather",
        )(*toks[:7], *weights[:3])
        send, tok, _, wts = pl.pallas_call(
            first_kernel,
            out_shape=(half, token_half, token_half, blocks),
            in_specs=[VMEM] * 7,
            out_specs=(VMEM,) * 4,
            input_output_aliases={4: 1, 5: 2, 6: 3},
            compiler_params=pltpu.CompilerParams(vmem_limit_bytes=8 << 20),
            cost_estimate=pl.CostEstimate(flops=m * t * k, bytes_accessed=2 * k * (m + t), transcendentals=0),
            name="first",
        )(*toks[7:], *weights[3:], *placed)
        keep = pl.pallas_call(
            half_product,
            out_shape=half,
            in_specs=[VMEM] * 2,
            out_specs=VMEM,
            compiler_params=pltpu.CompilerParams(vmem_limit_bytes=8 << 20),
            cost_estimate=pl.CostEstimate(flops=m * t * k, bytes_accessed=2 * k * (m + t), transcendentals=0),
            name="keep",
        )(tok, wts)
        whole = (keep + core_swap(send)).reshape(4, 2, units, t // 2)
        g, u = whole[:, 0], whole[:, 1]
        hidden = (jax.nn.silu(g) * u).astype(bf16).reshape(4 * units, t // 2)

        hids = z_direct(hidden)
        piece = jax.ShapeDtypeStruct((n, 2 * PAD), bf16)
        shares = pl.pallas_call(
            second_kernel,
            out_shape=(piece,) * 4,
            in_specs=[VMEM] * 11,
            out_specs=(VMEM,) * 4,
            scratch_shapes=[pltpu.VMEM((Z * 4 * units, t // 2), bf16), pltpu.VMEM((t // 2, 2 * PAD), jnp.float32)],
            compiler_params=pltpu.CompilerParams(vmem_limit_bytes=10 << 20),
            cost_estimate=pl.CostEstimate(flops=2 * Z * 4 * units * t * PAD, bytes_accessed=6 << 20, transcendentals=0),
            name="second",
        )(*hids, near, far)

        parts = shares[0], py(shares[1], 1), py(shares[2], 2), py(shares[3], -1)
        total = sum(p.astype(jnp.float32) for p in parts).astype(bf16)
        mine, other = (lax.dynamic_slice_in_dim(total, d * PAD, PAD, 1) for d in (xh, 1 - xh))
        got_a, got_b = lax.ppermute(mine, final_axes, final_perms[0]), lax.ppermute(other, final_axes, final_perms[1])
        return pl.pallas_call(
            out_kernel,
            out_shape=jax.ShapeDtypeStruct((down.shape[1], 2 * n), bf16),
            in_specs=[VMEM] * 2,
            out_specs=VMEM,
            compiler_params=pltpu.CompilerParams(vmem_limit_bytes=4 << 20),
            name="out",
        )(got_a, got_b).T

    row, col = ("z", "xl"), ("y", "xh")
    return jax.shard_map(
        body,
        mesh=grid,
        in_specs=(P(row, "c"), P(col + row, "c"), P(col + row, "c"), P(col + ("c",), row)),
        out_specs=P(row, col + ("c",)),
        check_vma=False,
    )
```
